32 devices in a mesh: req: 2 (over core), seq: 16 (over z, y, x).
Axes of the slice: x: 2, y: 2, z: 4, core: 2. Of those that a mesh axis runs over, the one named last changes fastest.
Arguments:
- image_query: bfloat16 [256, 1536], P(('req', 'seq')), parts along dimension 0, may hold values from -6 to 6
- image_key: bfloat16 [256, 1536], P(('req', 'seq')), parts along dimension 0, may hold values from -6 to 6
- image_value: bfloat16 [256, 1536], P(('req', 'seq')), parts along dimension 0, may hold values from -6 to 6
- text_query: bfloat16 [1024, 1536], P('req'), parts along dimension 0, may hold values from -6 to 6
- text_key: bfloat16 [1024, 1536], P('req'), parts along dimension 0, may hold values from -6 to 6
- text_value: bfloat16 [1024, 1536], P('req'), parts along dimension 0, may hold values from -6 to 6
- image_query_gain: float32 [128], replicated, may hold values from 1 to 8
- image_key_gain: float32 [128], replicated, may hold values from 1 to 8
- text_query_gain: float32 [128], replicated, may hold values from 1 to 2.5
- text_key_gain: float32 [128], replicated, may hold values from 1 to 2.5
- image_order: int32 [256], P(('req', 'seq')), parts along dimension 0, may hold values from 0 to 127, each once
- text_length: int32 [2], P('req'), parts along dimension 0, may hold values from 256 to 512
Outputs:
- image_out: bfloat16 [256, 1536], P(('req', 'seq')), parts along dimension 0
- text_out: bfloat16 [1024, 1536], P(('req', 'seq')), parts along dimension 0
The draws below stay inside these ranges and needn't reach their ends.
There are 2 independent parts, one for each index of `req`. The reference program is written for one: setup_inputs(seed, part) draws one part's arguments, and reference() takes and returns one part's arrays. A program takes and returns all parts, laid end to end along the dimension named above; an argument that names none is the same for every part. Nothing has to cross between parts.
Inputs may be any that keep to these rules, and one draw needn't show every extreme that they name: `image_order`: every position 0 to 127 appears once.
All inputs are finite; a program needn't handle non-finite values.
Results may differ from the reference program's by a relative error of at most 0.005.
The reference program's roundings to bfloat16 on the way (of `weights`) count: a program that leaves them out, or rounds other values in their place, can miss the bound.
Values may be sent and summed in bfloat16 or wider, within the bound.
A program may use at most 64 MiB of HBM per device.

```python
import jax
import jax.numpy as jnp
from jax import lax

H = 12
HD = 128
TXT = 512
GRID_W = 64
TOK_DEV = 8
IMG = 128
N_SEQ = 16


def draw_image_query(key, part):
    queries = jax.random.normal(jax.random.fold_in(key, 1), (IMG, H * HD), jnp.float32)
    return jnp.clip(queries, -6.0, 6.0).astype(jnp.bfloat16)


def draw_image_key(key, part):
    keys_drawn = jax.random.normal(jax.random.fold_in(key, 2), (IMG, H * HD), jnp.float32)
    return jnp.clip(keys_drawn, -6.0, 6.0).astype(jnp.bfloat16)


def draw_image_query_gain(key, part):
    return jax.random.uniform(jax.random.fold_in(key, 5), (HD,), jnp.float32, 1.0, 2.5)


def draw_image_key_gain(key, part):
    return jax.random.uniform(jax.random.fold_in(key, 6), (HD,), jnp.float32, 1.0, 2.5)


def level_of(own_key, dims, cuts, low, top_value):
    level, own = 1.0, jax.random.fold_in(own_key, 6)
    for dim, parts in cuts:
        heights = jnp.exp(jax.random.uniform(jax.random.fold_in(own, dim), (parts,), jnp.float32, low / len(cuts), top_value / len(cuts)))
        level = level * jnp.repeat(heights, dims[dim] // parts).reshape([-1 if axis == dim else 1 for axis in range(len(dims))])
    return level


def bell_draw(stream_key, dims, deviation, limit, pieces=(), held_as=jnp.bfloat16):
    level = level_of(stream_key, dims, pieces, -0.22, 0.18) if pieces else 1.0
    values = jax.random.normal(stream_key, dims, jnp.float32) * deviation * level
    return jnp.minimum(jnp.maximum(values, -limit), limit).astype(held_as)


def setup_inputs(seed: int = 0, part: int = 0) -> dict:
    key_of = jax.random.split(jax.random.key(seed), 13)
    part_keys = jax.random.split(jax.random.fold_in(key_of[12], part), 13)
    image_query = draw_image_query(jax.random.fold_in(jax.random.fold_in(key_of[12], part), 71), part)
    image_key = draw_image_key(jax.random.fold_in(jax.random.fold_in(key_of[12], part), 71), part)
    image_value = bell_draw(part_keys[2], (IMG, H * HD), 1.0, 6.0, ((0, 16),))
    text_query = bell_draw(part_keys[3], (TXT, H * HD), 1.0, 6.0)
    text_key = bell_draw(part_keys[4], (TXT, H * HD), 1.0, 6.0)
    text_value = bell_draw(part_keys[5], (TXT, H * HD), 1.0, 6.0)
    image_query_gain = draw_image_query_gain(jax.random.fold_in(key_of[12], 71), part)
    image_key_gain = draw_image_key_gain(jax.random.fold_in(key_of[12], 71), part)
    text_query_gain = jnp.clip(jax.random.uniform(key_of[8], (HD,), jnp.float32, 1.0, 2.5), 1.0, 2.5)
    text_key_gain = jnp.clip(jax.random.uniform(key_of[9], (HD,), jnp.float32, 1.0, 2.5), 1.0, 2.5)
    image_order = jax.random.permutation(part_keys[10], IMG).astype(jnp.int32)
    text_length = jax.random.randint(part_keys[11], (1,), TXT // 2, TXT + 1).astype(jnp.int32)
    return {"image_query": image_query, "image_key": image_key, "image_value": image_value, "text_query": text_query, "text_key": text_key, "text_value": text_value, "image_query_gain": image_query_gain, "image_key_gain": image_key_gain, "text_query_gain": text_query_gain, "text_key_gain": text_key_gain, "image_order": image_order, "text_length": text_length}


epsilon = 1e-06
masked_score = -1e+30

def head_norm(values, norm_gain, head_count):
    row_count = values.shape[0]
    shaped = values.astype(jnp.float32).reshape(row_count, head_count, -1)
    mean_square = lax.optimization_barrier(jnp.mean(shaped * shaped, axis=-1, keepdims=True))
    return shaped * lax.rsqrt(mean_square + epsilon) * norm_gain

def rotate(normed, positions, half_length):
    row_count, head_count, head_dim = normed.shape
    pair_count = head_dim // 2
    pair_ids = jnp.arange(pair_count)
    first_axis = pair_ids < 8
    second = pair_ids < 36
    within = jnp.where(first_axis, pair_ids, jnp.where(second, pair_ids - 8, pair_ids - 36)).astype(jnp.float32)
    axis_dim = jnp.where(first_axis, 16.0, 56.0).astype(jnp.float32)
    frequency = jnp.power(jnp.float32(10000.0), -2.0 * within / axis_dim)
    image_index = positions // half_length
    inside = positions % half_length
    row_place = inside // GRID_W
    column_place = inside % GRID_W
    coordinate = jnp.where(first_axis[None, :], image_index[:, None], jnp.where(second[None, :], row_place[:, None], column_place[:, None])).astype(jnp.float32)
    angles = coordinate * frequency[None, :]
    cosine = jnp.cos(angles)[:, None, :]
    sine_part = jnp.sin(angles)[:, None, :]
    paired = normed.reshape(row_count, head_count, pair_count, 2)
    even_part = paired[..., 0]
    odd_part = paired[..., 1]
    turned = jnp.stack([even_part * cosine - odd_part * sine_part, even_part * sine_part + odd_part * cosine], axis=-1)
    return turned.reshape(row_count, head_count * head_dim)

def reference(image_query, image_key, image_value, text_query, text_key, text_value, image_query_gain, image_key_gain, text_query_gain, text_key_gain, image_order, text_length):
    head_count = image_query.shape[1] // HD
    half_length = IMG // 2
    query_img = lax.optimization_barrier(rotate(head_norm(image_query, image_query_gain, head_count), image_order, half_length).astype(jnp.bfloat16))
    key_img = lax.optimization_barrier(rotate(head_norm(image_key, image_key_gain, head_count), image_order, half_length).astype(jnp.bfloat16))
    query_txt = lax.optimization_barrier(head_norm(text_query, text_query_gain, head_count).reshape(TXT, -1).astype(jnp.bfloat16))
    key_txt = lax.optimization_barrier(head_norm(text_key, text_key_gain, head_count).reshape(TXT, -1).astype(jnp.bfloat16))
    all_keys = jnp.concatenate([key_txt, key_img], axis=0).astype(jnp.float32)
    all_values = jnp.concatenate([text_value, image_value], axis=0).astype(jnp.float32)
    key_count = all_keys.shape[0]
    key_heads = all_keys.reshape(key_count, head_count, HD)
    value_heads = all_values.reshape(key_count, head_count, HD)
    valid = jnp.concatenate([jnp.arange(TXT) < text_length[0], jnp.ones((IMG,), dtype=bool)])
    scaling = HD ** (-0.5)

    def attend(block):
        row_count = block.shape[0]
        query_heads = block.astype(jnp.float32).reshape(row_count, head_count, HD)
        scores = jnp.einsum('rhd,shd->rhs', query_heads, key_heads) * scaling
        scores = jnp.where(valid[None, None, :], scores, masked_score)
        row_max = lax.optimization_barrier(jnp.max(scores, axis=-1))
        expo = jnp.exp(scores - row_max[..., None])
        expo = jnp.where(valid[None, None, :], expo, 0.0)
        totals = lax.optimization_barrier(jnp.sum(expo, axis=-1))
        weights = lax.optimization_barrier(expo.astype(jnp.bfloat16)).astype(jnp.float32)
        blended = jnp.einsum('rhs,shd->rhd', weights, value_heads)
        return (blended / totals[..., None]).reshape(row_count, -1).astype(jnp.bfloat16)
    text_out = lax.map(attend, query_txt.reshape(N_SEQ, TXT // N_SEQ, -1)).reshape(TXT, -1)
    image_out = lax.map(attend, query_img.reshape(N_SEQ, TOK_DEV, -1)).reshape(IMG, -1)
    return (image_out, text_out)
```

```python
import functools
import math

import jax
import jax.numpy as jnp
from jax import lax
from jax.experimental import pallas as pl
from jax.experimental.pallas import tpu as pltpu
from jax.sharding import PartitionSpec as P

GRID_W = 64
EPS = 1e-06
LOW = -1e30
MESH = pl.DeviceIdType.MESH


def line_sizes(devices):
    z_size = 4 if devices % 4 == 0 else 1
    rest = devices // z_size
    x_size = 1
    while x_size * x_size * 4 <= rest and rest % (x_size * 2) == 0:
        x_size *= 2
    return z_size, rest // x_size, x_size


def rsqrt_mean(values):
    return lax.rsqrt(jnp.mean(values * values, axis=-1, keepdims=True) + EPS)


def kernel(
    devices,
    iq_ref,
    ik_ref,
    iv_ref,
    tq_ref,
    tk_ref,
    tv_ref,
    iqg_ref,
    ikg_ref,
    tqg_ref,
    tkg_ref,
    order_ref,
    length_ref,
    io_ref,
    to_ref,
    kbuf,
    vbuf,
    tq_buf,
    tk_buf,
    tv_buf,
    qs,
    m_buf,
    l_buf,
    o_buf,
    recv_sem,
    send_sem,
    local_sem,
):
    zs, ys, xs = line_sizes(devices)
    me = lax.axis_index("seq")
    req = lax.axis_index("req")
    x_me = me % xs
    y_me = (me // xs) % ys
    z_me = me // (xs * ys)

    def block(z, y, x):
        return (z * ys + y) * xs + x

    if zs == 4:
        z_others = [z_me + 1 - 2 * (z_me % 2), 3 - z_me, (z_me + 2) % 4]
    else:
        z_others = []
    y_others = [(y_me + d) % ys for d in range(1, ys)]
    x_others = [(x_me + d) % xs for d in range(1, xs)]
    z_peers = [block(z, y_me, x_me) for z in z_others]
    y_peers = [block(z_me, y, x_me) for y in y_others]
    x_peers = [block(z_me, y_me, x) for x in x_others]
    peers = z_peers + y_peers + x_peers

    barrier = pltpu.get_barrier_semaphore()
    for peer in peers:
        pl.semaphore_signal(barrier, inc=1, device_id=(req, peer), device_id_type=MESH)

    own_rows, width = iq_ref.shape
    size = iqg_ref.shape[-1]
    heads = width // size
    share = tq_buf.shape[0]
    text_rows = tk_ref.shape[0]
    rows = share + own_rows
    groups = tk_buf.shape[0]
    per = heads // groups
    span = per * size
    scale = math.log2(math.e) / math.sqrt(size)

    tq_copy = pltpu.make_async_copy(
        tq_ref.at[pl.ds(pl.multiple_of(me * share, share), share), :],
        tq_buf,
        local_sem.at[2 * groups],
    )
    tq_copy.start()
    text_copies = []
    for g in range(groups):
        pair = (
            pltpu.make_async_copy(
                tk_ref.at[:, pl.ds(g * span, span)], tk_buf.at[g], local_sem.at[2 * g]
            ),
            pltpu.make_async_copy(
                tv_ref.at[:, pl.ds(g * span, span)], tv_buf.at[g], local_sem.at[2 * g + 1]
            ),
        )
        for copy in pair:
            copy.start()
        text_copies.append(pair)

    half_length = own_rows * devices // 2
    lane = lax.broadcasted_iota(jnp.int32, (own_rows, size), 1)
    row = lax.broadcasted_iota(jnp.int32, (own_rows, size), 0)
    pair_id = lane // 2
    first = pair_id < 8
    second = pair_id < 36
    coordinate = jnp.zeros((own_rows, size), jnp.int32)
    for r in range(own_rows):
        position = order_ref[r]
        inside = position % half_length
        here = jnp.where(
            first,
            position // half_length,
            jnp.where(second, inside // GRID_W, inside % GRID_W),
        )
        coordinate = jnp.where(row == r, here, coordinate)
    within = jnp.where(first, pair_id, jnp.where(second, pair_id - 8, pair_id - 36))
    step = jnp.where(first, 2.0 / 16.0, 2.0 / 56.0) * (-math.log(10000.0))
    angle = coordinate.astype(jnp.float32) * jnp.exp(within.astype(jnp.float32) * step)
    cosine = jnp.cos(angle)
    sine = jnp.sin(angle)
    even = lane % 2 == 0
    sine = jnp.where(even, -sine, sine)

    def turned(values, gain):
        normed = values * rsqrt_mean(values) * gain
        swapped = jnp.where(
            even, pltpu.roll(normed, size - 1, 1), pltpu.roll(normed, 1, 1)
        )
        return normed * cosine + swapped * sine

    for h in range(heads):
        cols = slice(h * size, (h + 1) * size)
        key = turned(ik_ref[:, cols].astype(jnp.float32), ikg_ref[...])
        kbuf[me, :, cols] = key.astype(jnp.bfloat16)
    vbuf[me] = iv_ref[...]

    pl.semaphore_wait(barrier, len(peers))

    count = [0]
    sends = []

    def send(kind, idx, peer, source=None):
        buf = (kbuf, vbuf)[kind]
        copy = pltpu.make_async_remote_copy(
            src_ref=buf.at[idx] if source is None else source,
            dst_ref=buf.at[idx],
            send_sem=send_sem.at[count[0]],
            recv_sem=recv_sem.at[kind, idx],
            device_id=(req, peer),
            device_id_type=MESH,
        )
        count[0] += 1
        copy.start()
        sends.append(copy)

    def arrive(kind, idx):
        buf = (kbuf, vbuf)[kind]
        pltpu.make_async_remote_copy(
            src_ref=buf.at[idx],
            dst_ref=buf.at[idx],
            send_sem=send_sem.at[0],
            recv_sem=recv_sem.at[kind, idx],
            device_id=(req, me),
            device_id_type=MESH,
        ).wait_recv()

    for group in (z_peers, y_peers, x_peers):
        for peer in group:
            send(1, me, peer, iv_ref)
            send(0, me, peer)

    def near_plane():
        for y in y_others:
            idx = block(z_me, y, x_me)
            arrive(0, idx)
            for peer in x_peers:
                send(0, idx, peer)
        for x in x_others:
            idx = block(z_me, y_me, x)
            arrive(1, idx)
            for peer in y_peers:
                send(1, idx, peer)

    def far_column(z):
        idx = block(z, y_me, x_me)
        for kind in (0, 1):
            arrive(kind, idx)
            for peer in y_peers + x_peers:
                send(kind, idx, peer)

    def far_plane(z):
        for y in y_others:
            idx = block(z, y, x_me)
            arrive(0, idx)
            for peer in x_peers:
                send(0, idx, peer)
        for x in x_others:
            idx = block(z, y_me, x)
            arrive(1, idx)
            for peer in y_peers:
                send(1, idx, peer)

    stages = [[] for _ in range(groups)]
    tasks = [near_plane]
    tasks += [functools.partial(far_column, z) for z in z_others]
    tasks += [functools.partial(far_plane, z) for z in z_others]
    for i, task in enumerate(tasks):
        stages[min(i * groups // len(tasks), groups - 1)].append(task)

    tq_copy.wait()
    for h in range(heads):
        cols = slice(h * size, (h + 1) * size)
        text = tq_buf[:, cols].astype(jnp.float32)
        text = text * rsqrt_mean(text) * tqg_ref[...]
        image = turned(iq_ref[:, cols].astype(jnp.float32), iqg_ref[...])
        qs[h] = jnp.concatenate([text, image], axis=0).astype(jnp.bfloat16)

    valid = lax.broadcasted_iota(jnp.int32, (rows, text_rows), 1) < length_ref[0]

    def scores_of(query, key):
        return (
            lax.dot_general(
                query, key, (((1,), (1,)), ((), ())), preferred_element_type=jnp.float32
            )
            * scale
        )

    for g in range(groups):
        for copy in text_copies[g]:
            copy.wait()
        for i in range(per):
            h = g * per + i
            cols = slice(i * size, (i + 1) * size)
            key = tk_buf[g, :, cols].astype(jnp.float32)
            key = (key * rsqrt_mean(key) * tkg_ref[...]).astype(jnp.bfloat16)
            scores = jnp.where(valid, scores_of(qs[h], key), LOW)
            top = jnp.max(scores, axis=-1, keepdims=True)
            expo = jnp.where(valid, jnp.exp2(scores - top), 0.0)
            m_buf[h] = jnp.broadcast_to(top, (rows, size))
            l_buf[h] = jnp.broadcast_to(jnp.sum(expo, axis=-1, keepdims=True), (rows, size))
            o_buf[h] = jnp.dot(
                expo.astype(jnp.bfloat16),
                tv_buf[g, :, cols],
                preferred_element_type=jnp.float32,
            )
        for task in stages[g]:
            task()

    for z in [z_me] + z_others:
        for y in [y_me] + y_others:
            for x in x_others:
                arrive(0, block(z, y, x))
        for x in [x_me] + x_others:
            for y in y_others:
                arrive(1, block(z, y, x))

    for h in range(heads):
        cols = slice(h * size, (h + 1) * size)
        key = kbuf[:, :, cols].astype(jnp.float32).reshape(devices * own_rows, size)
        value = vbuf[:, :, cols].astype(jnp.float32).reshape(devices * own_rows, size)
        scores = scores_of(qs[h], key.astype(jnp.bfloat16))
        old = m_buf[h][:, :1]
        top = jnp.maximum(old, jnp.max(scores, axis=-1, keepdims=True))
        expo = jnp.exp2(scores - top)
        back = jnp.exp2(old - top)
        total = l_buf[h][:, :1] * back + jnp.sum(expo, axis=-1, keepdims=True)
        out = o_buf[h] * back + jnp.dot(
            expo.astype(jnp.bfloat16),
            value.astype(jnp.bfloat16),
            preferred_element_type=jnp.float32,
        )
        out = out / total
        to_ref[:, cols] = out[:share].astype(jnp.bfloat16)
        io_ref[:, cols] = out[share:].astype(jnp.bfloat16)

    for copy in sends:
        copy.wait_send()


def send_count(devices):
    zs, ys, xs = line_sizes(devices)
    keys = (zs - 1) + zs * (ys - 1) + zs * ys * (xs - 1)
    values = (zs - 1) + zs * (xs - 1) + zs * xs * (ys - 1)
    return keys + values


def local(iq, ik, iv, tq, tk, tv, iqg, ikg, tqg, tkg, order, length):
    devices = lax.axis_size("seq")
    own_rows, width = iq.shape
    size = iqg.shape[0]
    heads = width // size
    text_rows = tq.shape[0]
    share = text_rows // devices
    rows = share + own_rows
    groups = heads // 2 if heads % 2 == 0 else heads
    span = width // groups
    vmem = pl.BlockSpec(memory_space=pltpu.VMEM)
    smem = pl.BlockSpec(memory_space=pltpu.SMEM)
    hbm = pl.BlockSpec(memory_space=pl.ANY)
    gains = [g.reshape(1, size) for g in (iqg, ikg, tqg, tkg)]
    return pl.pallas_call(
        functools.partial(kernel, devices),
        out_shape=(
            jax.ShapeDtypeStruct((own_rows, width), jnp.bfloat16),
            jax.ShapeDtypeStruct((share, width), jnp.bfloat16),
        ),
        in_specs=[vmem] * 3 + [hbm] * 3 + [vmem] * 4 + [smem] * 2,
        out_specs=(vmem, vmem),
        scratch_shapes=[
            pltpu.VMEM((devices, own_rows, width), jnp.bfloat16),
            pltpu.VMEM((devices, own_rows, width), jnp.bfloat16),
            pltpu.VMEM((share, width), jnp.bfloat16),
            pltpu.VMEM((groups, text_rows, span), jnp.bfloat16),
            pltpu.VMEM((groups, text_rows, span), jnp.bfloat16),
            pltpu.VMEM((heads, rows, size), jnp.bfloat16),
            pltpu.VMEM((heads, rows, size), jnp.float32),
            pltpu.VMEM((heads, rows, size), jnp.float32),
            pltpu.VMEM((heads, rows, size), jnp.float32),
            pltpu.SemaphoreType.DMA((2, devices)),
            pltpu.SemaphoreType.DMA((send_count(devices),)),
            pltpu.SemaphoreType.DMA((2 * groups + 1,)),
        ],
        compiler_params=pltpu.CompilerParams(
            collective_id=0, has_side_effects=True, vmem_limit_bytes=62 * 1024 * 1024
        ),
    )(iq, ik, iv, tq, tk, tv, *gains, order, length)


def solution(mesh):
    rows = P(("req", "seq"), None)
    text = P("req", None)
    return jax.shard_map(
        local,
        mesh=mesh,
        in_specs=(rows, rows, rows, text, text, text)
        + (P(), P(), P(), P(), P(("req", "seq")), P("req")),
        out_specs=(rows, rows),
        check_vma=False,
    )
```

```python
import functools
import math

import jax
import jax.numpy as jnp
from jax import lax
from jax.experimental import pallas as pl
from jax.experimental.pallas import tpu as pltpu
from jax.sharding import PartitionSpec as P

GRID_W = 64
EPS = 1e-06
LOW = -1e30
MESH = pl.DeviceIdType.MESH


def line_sizes(devices):
    z_size = 4 if devices % 4 == 0 else 1
    rest = devices // z_size
    x_size = 1
    while x_size * x_size * 4 <= rest and rest % (x_size * 2) == 0:
        x_size *= 2
    return z_size, rest // x_size, x_size


def rsqrt_mean(values):
    return lax.rsqrt(jnp.mean(values * values, axis=-1, keepdims=True) + EPS)


def kernel(
    devices,
    iq_ref,
    ik_ref,
    iv_ref,
    tq_ref,
    tk_ref,
    tv_ref,
    iqg_ref,
    ikg_ref,
    tqg_ref,
    tkg_ref,
    order_ref,
    length_ref,
    io_ref,
    to_ref,
    kbuf,
    vbuf,
    tq_buf,
    tk_buf,
    tv_buf,
    qs,
    m_buf,
    l_buf,
    o_buf,
    recv_sem,
    send_sem,
    local_sem,
):
    zs, ys, xs = line_sizes(devices)
    me = lax.axis_index("seq")
    req = lax.axis_index("req")
    x_me = me % xs
    y_me = (me // xs) % ys
    z_me = me // (xs * ys)

    def block(z, y, x):
        return (z * ys + y) * xs + x

    if zs == 4:
        z_others = [z_me + 1 - 2 * (z_me % 2), 3 - z_me, (z_me + 2) % 4]
    else:
        z_others = []
    y_others = [(y_me + d) % ys for d in range(1, ys)]
    x_others = [(x_me + d) % xs for d in range(1, xs)]
    z_peers = [block(z, y_me, x_me) for z in z_others]
    y_peers = [block(z_me, y, x_me) for y in y_others]
    x_peers = [block(z_me, y_me, x) for x in x_others]
    peers = z_peers + y_peers + x_peers

    barrier = pltpu.get_barrier_semaphore()
    for peer in peers:
        pl.semaphore_signal(barrier, inc=1, device_id=(req, peer), device_id_type=MESH)

    own_rows, width = iq_ref.shape
    size = iqg_ref.shape[-1]
    heads = width // size
    share = tq_buf.shape[0]
    text_rows = tk_ref.shape[0]
    rows = share + own_rows
    groups = tk_buf.shape[0]
    per = heads // groups
    span = per * size
    scale = math.log2(math.e) / math.sqrt(size)

    tq_copy = pltpu.make_async_copy(
        tq_ref.at[pl.ds(pl.multiple_of(me * share, share), share), :],
        tq_buf,
        local_sem.at[2 * groups],
    )
    tq_copy.start()
    text_copies = []
    for g in range(groups):
        pair = (
            pltpu.make_async_copy(
                tk_ref.at[:, pl.ds(g * span, span)], tk_buf.at[g], local_sem.at[2 * g]
            ),
            pltpu.make_async_copy(
                tv_ref.at[:, pl.ds(g * span, span)], tv_buf.at[g], local_sem.at[2 * g + 1]
            ),
        )
        for copy in pair:
            copy.start()
        text_copies.append(pair)

    half_length = own_rows * devices // 2
    lane = lax.broadcasted_iota(jnp.int32, (own_rows, size), 1)
    row = lax.broadcasted_iota(jnp.int32, (own_rows, size), 0)
    pair_id = lane // 2
    first = pair_id < 8
    second = pair_id < 36
    coordinate = jnp.zeros((own_rows, size), jnp.int32)
    for r in range(own_rows):
        position = order_ref[r]
        inside = position % half_length
        here = jnp.where(
            first,
            position // half_length,
            jnp.where(second, inside // GRID_W, inside % GRID_W),
        )
        coordinate = jnp.where(row == r, here, coordinate)
    within = jnp.where(first, pair_id, jnp.where(second, pair_id - 8, pair_id - 36))
    step = jnp.where(first, 2.0 / 16.0, 2.0 / 56.0) * (-math.log(10000.0))
    angle = coordinate.astype(jnp.float32) * jnp.exp(within.astype(jnp.float32) * step)
    cosine = jnp.cos(angle)
    sine = jnp.sin(angle)
    even = lane % 2 == 0
    sine = jnp.where(even, -sine, sine)

    def turned(values, gain):
        normed = values * rsqrt_mean(values) * gain
        swapped = jnp.where(
            even, pltpu.roll(normed, size - 1, 1), pltpu.roll(normed, 1, 1)
        )
        return normed * cosine + swapped * sine

    for h in range(heads):
        cols = slice(h * size, (h + 1) * size)
        key = turned(ik_ref[:, cols].astype(jnp.float32), ikg_ref[...])
        kbuf[me, :, cols] = key.astype(jnp.bfloat16)
    vbuf[me] = iv_ref[...]

    pl.semaphore_wait(barrier, len(peers))

    count = [0]
    sends = []

    def send(kind, idx, peer, source=None):
        buf = (kbuf, vbuf)[kind]
        copy = pltpu.make_async_remote_copy(
            src_ref=buf.at[idx] if source is None else source,
            dst_ref=buf.at[idx],
            send_sem=send_sem.at[count[0]],
            recv_sem=recv_sem.at[kind, idx],
            device_id=(req, peer),
            device_id_type=MESH,
        )
        count[0] += 1
        copy.start()
        sends.append(copy)

    def arrive(kind, idx):
        buf = (kbuf, vbuf)[kind]
        pltpu.make_async_remote_copy(
            src_ref=buf.at[idx],
            dst_ref=buf.at[idx],
            send_sem=send_sem.at[0],
            recv_sem=recv_sem.at[kind, idx],
            device_id=(req, me),
            device_id_type=MESH,
        ).wait_recv()

    for group in (z_peers, y_peers, x_peers):
        for peer in group:
            send(1, me, peer, iv_ref)
            send(0, me, peer)

    def near_plane():
        for y in y_others:
            idx = block(z_me, y, x_me)
            arrive(0, idx)
            for peer in x_peers:
                send(0, idx, peer)
        for x in x_others:
            idx = block(z_me, y_me, x)
            arrive(1, idx)
            for peer in y_peers:
                send(1, idx, peer)

    def far_column(z):
        idx = block(z, y_me, x_me)
        for kind in (0, 1):
            arrive(kind, idx)
            for peer in y_peers + x_peers:
                send(kind, idx, peer)

    def far_plane(z):
        for y in y_others:
            idx = block(z, y, x_me)
            arrive(0, idx)
            for peer in x_peers:
                send(0, idx, peer)
        for x in x_others:
            idx = block(z, y_me, x)
            arrive(1, idx)
            for peer in y_peers:
                send(1, idx, peer)

    stages = [[] for _ in range(groups)]
    tasks = [near_plane]
    tasks += [functools.partial(far_column, z) for z in z_others]
    tasks += [functools.partial(far_plane, z) for z in z_others]
    for i, task in enumerate(tasks):
        stages[min(i * groups // len(tasks), groups - 1)].append(task)

    tq_copy.wait()
    for h in range(heads):
        cols = slice(h * size, (h + 1) * size)
        text = tq_buf[:, cols].astype(jnp.float32)
        text = text * rsqrt_mean(text) * tqg_ref[...]
        image = turned(iq_ref[:, cols].astype(jnp.float32), iqg_ref[...])
        qs[h] = jnp.concatenate([text, image], axis=0).astype(jnp.bfloat16)

    valid = lax.broadcasted_iota(jnp.int32, (rows, text_rows), 1) < length_ref[0]

    def scores_of(query, key):
        return (
            lax.dot_general(
                query, key, (((1,), (1,)), ((), ())), preferred_element_type=jnp.float32
            )
            * scale
        )

    for g in range(groups):
        for copy in text_copies[g]:
            copy.wait()
        for i in range(per):
            h = g * per + i
            cols = slice(i * size, (i + 1) * size)
            key = tk_buf[g, :, cols].astype(jnp.float32)
            key = (key * rsqrt_mean(key) * tkg_ref[...]).astype(jnp.bfloat16)
            scores = jnp.where(valid, scores_of(qs[h], key), LOW)
            top = jnp.max(scores, axis=-1, keepdims=True)
            expo = jnp.where(valid, jnp.exp2(scores - top), 0.0)
            m_buf[h] = jnp.broadcast_to(top, (rows, size))
            l_buf[h] = jnp.broadcast_to(jnp.sum(expo, axis=-1, keepdims=True), (rows, size))
            o_buf[h] = jnp.dot(
                expo.astype(jnp.bfloat16),
                tv_buf[g, :, cols],
                preferred_element_type=jnp.float32,
            )
        for task in stages[g]:
            task()

    for z in [z_me] + z_others:
        for y in [y_me] + y_others:
            for x in x_others:
                arrive(0, block(z, y, x))
        for x in [x_me] + x_others:
            for y in y_others:
                arrive(1, block(z, y, x))

    def lanes(h):
        return slice(h * size, (h + 1) * size)

    def gathered(buf, h):
        whole = buf[:, :, lanes(h)].astype(jnp.float32)
        return whole.reshape(devices * own_rows, size).astype(jnp.bfloat16)

    every = range(heads)
    scores = [scores_of(qs[h], gathered(kbuf, h)) for h in every]
    olds = [m_buf[h] for h in every]
    tops = [
        jnp.maximum(olds[h][:, :1], jnp.max(scores[h], axis=-1, keepdims=True))
        for h in every
    ]
    expos = [jnp.exp2(scores[h] - tops[h]) for h in every]
    added = [
        jnp.dot(
            expos[h].astype(jnp.bfloat16),
            gathered(vbuf, h),
            preferred_element_type=jnp.float32,
        )
        for h in every
    ]
    sums = [jnp.sum(expos[h], axis=-1, keepdims=True) for h in every]
    for h in every:
        back = jnp.exp2(olds[h] - tops[h])
        out = (o_buf[h] * back + added[h]) / (l_buf[h] * back + sums[h])
        to_ref[:, lanes(h)] = out[:share].astype(jnp.bfloat16)
        io_ref[:, lanes(h)] = out[share:].astype(jnp.bfloat16)

    for copy in sends:
        copy.wait_send()


def send_count(devices):
    zs, ys, xs = line_sizes(devices)
    keys = (zs - 1) + zs * (ys - 1) + zs * ys * (xs - 1)
    values = (zs - 1) + zs * (xs - 1) + zs * xs * (ys - 1)
    return keys + values


def local(iq, ik, iv, tq, tk, tv, iqg, ikg, tqg, tkg, order, length):
    devices = lax.axis_size("seq")
    own_rows, width = iq.shape
    size = iqg.shape[0]
    heads = width // size
    text_rows = tq.shape[0]
    share = text_rows // devices
    rows = share + own_rows
    groups = heads // 2 if heads % 2 == 0 else heads
    span = width // groups
    vmem = pl.BlockSpec(memory_space=pltpu.VMEM)
    smem = pl.BlockSpec(memory_space=pltpu.SMEM)
    hbm = pl.BlockSpec(memory_space=pl.ANY)
    gains = [g.reshape(1, size) for g in (iqg, ikg, tqg, tkg)]
    return pl.pallas_call(
        functools.partial(kernel, devices),
        out_shape=(
            jax.ShapeDtypeStruct((own_rows, width), jnp.bfloat16),
            jax.ShapeDtypeStruct((share, width), jnp.bfloat16),
        ),
        in_specs=[vmem] * 3 + [hbm] * 3 + [vmem] * 4 + [smem] * 2,
        out_specs=(vmem, vmem),
        scratch_shapes=[
            pltpu.VMEM((devices, own_rows, width), jnp.bfloat16),
            pltpu.VMEM((devices, own_rows, width), jnp.bfloat16),
            pltpu.VMEM((share, width), jnp.bfloat16),
            pltpu.VMEM((groups, text_rows, span), jnp.bfloat16),
            pltpu.VMEM((groups, text_rows, span), jnp.bfloat16),
            pltpu.VMEM((heads, rows, size), jnp.bfloat16),
            pltpu.VMEM((heads, rows, size), jnp.float32),
            pltpu.VMEM((heads, rows, size), jnp.float32),
            pltpu.VMEM((heads, rows, size), jnp.float32),
            pltpu.SemaphoreType.DMA((2, devices)),
            pltpu.SemaphoreType.DMA((send_count(devices),)),
            pltpu.SemaphoreType.DMA((2 * groups + 1,)),
        ],
        compiler_params=pltpu.CompilerParams(
            collective_id=0, has_side_effects=True, vmem_limit_bytes=62 * 1024 * 1024
        ),
    )(iq, ik, iv, tq, tk, tv, *gains, order, length)


def solution(mesh):
    rows = P(("req", "seq"), None)
    text = P("req", None)
    return jax.shard_map(
        local,
        mesh=mesh,
        in_specs=(rows, rows, rows, text, text, text)
        + (P(), P(), P(), P(), P(("req", "seq")), P("req")),
        out_specs=(rows, rows),
        check_vma=False,
    )
```

```python
import functools
import math

import jax
import jax.numpy as jnp
from jax import lax
from jax.experimental import pallas as pl
from jax.experimental.pallas import tpu as pltpu
from jax.sharding import PartitionSpec as P

GRID_W = 64
EPS = 1e-06
LOW = -1e30
MESH = pl.DeviceIdType.MESH


def line_sizes(devices):
    z_size = 4 if devices % 4 == 0 else 1
    rest = devices // z_size
    x_size = 1
    while x_size * x_size * 4 <= rest and rest % (x_size * 2) == 0:
        x_size *= 2
    return z_size, rest // x_size, x_size


def rsqrt_mean(values):
    return lax.rsqrt(jnp.mean(values * values, axis=-1, keepdims=True) + EPS)


def kernel(
    devices,
    iq_ref,
    ik_ref,
    iv_ref,
    tq_ref,
    tk_ref,
    tv_ref,
    iqg_ref,
    ikg_ref,
    tqg_ref,
    tkg_ref,
    order_ref,
    length_ref,
    io_ref,
    to_ref,
    kbuf,
    vbuf,
    tq_buf,
    tk_buf,
    tv_buf,
    qs,
    m_buf,
    l_buf,
    o_buf,
    recv_sem,
    send_sem,
    local_sem,
):
    zs, ys, xs = line_sizes(devices)
    me = lax.axis_index("seq")
    req = lax.axis_index("req")
    x_me = me % xs
    y_me = (me // xs) % ys
    z_me = me // (xs * ys)

    def block(z, y, x):
        return (z * ys + y) * xs + x

    if zs == 4:
        z_others = [z_me + 1 - 2 * (z_me % 2), 3 - z_me, (z_me + 2) % 4]
    else:
        z_others = []
    y_others = [(y_me + d) % ys for d in range(1, ys)]
    x_others = [(x_me + d) % xs for d in range(1, xs)]
    z_peers = [block(z, y_me, x_me) for z in z_others]
    y_peers = [block(z_me, y, x_me) for y in y_others]
    x_peers = [block(z_me, y_me, x) for x in x_others]
    peers = z_peers + y_peers + x_peers

    barrier = pltpu.get_barrier_semaphore()
    for peer in peers:
        pl.semaphore_signal(barrier, inc=1, device_id=(req, peer), device_id_type=MESH)

    own_rows, width = iq_ref.shape
    size = iqg_ref.shape[-1]
    heads = width // size
    share = tq_buf.shape[0]
    text_rows = tk_ref.shape[0]
    rows = share + own_rows
    groups = tk_buf.shape[0]
    per = heads // groups
    span = per * size
    scale = math.log2(math.e) / math.sqrt(size)

    tq_copy = pltpu.make_async_copy(
        tq_ref.at[pl.ds(pl.multiple_of(me * share, share), share), :],
        tq_buf,
        local_sem.at[2 * groups],
    )
    tq_copy.start()
    text_copies = []
    for g in range(groups):
        pair = (
            pltpu.make_async_copy(
                tk_ref.at[:, pl.ds(g * span, span)], tk_buf.at[g], local_sem.at[2 * g]
            ),
            pltpu.make_async_copy(
                tv_ref.at[:, pl.ds(g * span, span)], tv_buf.at[g], local_sem.at[2 * g + 1]
            ),
        )
        for copy in pair:
            copy.start()
        text_copies.append(pair)

    half_length = own_rows * devices // 2
    lane = lax.broadcasted_iota(jnp.int32, (own_rows, size), 1)
    row = lax.broadcasted_iota(jnp.int32, (own_rows, size), 0)
    pair_id = lane // 2
    first = pair_id < 8
    second = pair_id < 36
    coordinate = jnp.zeros((own_rows, size), jnp.int32)
    for r in range(own_rows):
        position = order_ref[r]
        inside = position % half_length
        here = jnp.where(
            first,
            position // half_length,
            jnp.where(second, inside // GRID_W, inside % GRID_W),
        )
        coordinate = jnp.where(row == r, here, coordinate)
    within = jnp.where(first, pair_id, jnp.where(second, pair_id - 8, pair_id - 36))
    step = jnp.where(first, 2.0 / 16.0, 2.0 / 56.0) * (-math.log(10000.0))
    angle = coordinate.astype(jnp.float32) * jnp.exp(within.astype(jnp.float32) * step)
    cosine = jnp.cos(angle)
    sine = jnp.sin(angle)
    even = lane % 2 == 0
    sine = jnp.where(even, -sine, sine)

    def turned(values, gain):
        normed = values * rsqrt_mean(values) * gain
        swapped = jnp.where(
            even, pltpu.roll(normed, size - 1, 1), pltpu.roll(normed, 1, 1)
        )
        return normed * cosine + swapped * sine

    raw = [
        ik_ref[:, h * size : (h + 1) * size].astype(jnp.float32) for h in range(heads)
    ]
    inverse = [rsqrt_mean(part) for part in raw]
    normed = [part * inv * ikg_ref[...] for part, inv in zip(raw, inverse)]
    right = [pltpu.roll(part, size - 1, 1) for part in normed]
    left = [pltpu.roll(part, 1, 1) for part in normed]
    keys = [
        part * cosine + jnp.where(even, r, l) * sine
        for part, r, l in zip(normed, right, left)
    ]
    for h in range(heads):
        kbuf[me, :, h * size : (h + 1) * size] = keys[h].astype(jnp.bfloat16)
    vbuf[me] = iv_ref[...]

    pl.semaphore_wait(barrier, len(peers))

    count = [0]
    sends = []

    def send(kind, idx, peer, source=None):
        buf = (kbuf, vbuf)[kind]
        copy = pltpu.make_async_remote_copy(
            src_ref=buf.at[idx] if source is None else source,
            dst_ref=buf.at[idx],
            send_sem=send_sem.at[count[0]],
            recv_sem=recv_sem.at[kind, idx],
            device_id=(req, peer),
            device_id_type=MESH,
        )
        count[0] += 1
        copy.start()
        sends.append(copy)

    def arrive(kind, idx):
        buf = (kbuf, vbuf)[kind]
        pltpu.make_async_remote_copy(
            src_ref=buf.at[idx],
            dst_ref=buf.at[idx],
            send_sem=send_sem.at[0],
            recv_sem=recv_sem.at[kind, idx],
            device_id=(req, me),
            device_id_type=MESH,
        ).wait_recv()

    for group in (z_peers, y_peers, x_peers):
        for peer in group:
            send(1, me, peer, iv_ref)
            send(0, me, peer)

    def near_plane():
        for y in y_others:
            idx = block(z_me, y, x_me)
            arrive(0, idx)
            for peer in x_peers:
                send(0, idx, peer)
        for x in x_others:
            idx = block(z_me, y_me, x)
            arrive(1, idx)
            for peer in y_peers:
                send(1, idx, peer)

    def far_column(z):
        idx = block(z, y_me, x_me)
        for kind in (0, 1):
            arrive(kind, idx)
            for peer in y_peers + x_peers:
                send(kind, idx, peer)

    def far_plane(z):
        for y in y_others:
            idx = block(z, y, x_me)
            arrive(0, idx)
            for peer in x_peers:
                send(0, idx, peer)
        for x in x_others:
            idx = block(z, y_me, x)
            arrive(1, idx)
            for peer in y_peers:
                send(1, idx, peer)

    stages = [[] for _ in range(groups)]
    tasks = [near_plane]
    tasks += [functools.partial(far_column, z) for z in z_others]
    tasks += [functools.partial(far_plane, z) for z in z_others]
    for i, task in enumerate(tasks):
        stages[min(i * groups // len(tasks), groups - 1)].append(task)

    tq_copy.wait()
    for h in range(heads):
        cols = slice(h * size, (h + 1) * size)
        text = tq_buf[:, cols].astype(jnp.float32)
        text = text * rsqrt_mean(text) * tqg_ref[...]
        image = turned(iq_ref[:, cols].astype(jnp.float32), iqg_ref[...])
        qs[h] = jnp.concatenate([text, image], axis=0).astype(jnp.bfloat16)

    valid = lax.broadcasted_iota(jnp.int32, (rows, text_rows), 1) < length_ref[0]

    def scores_of(query, key):
        return (
            lax.dot_general(
                query, key, (((1,), (1,)), ((), ())), preferred_element_type=jnp.float32
            )
            * scale
        )

    for g in range(groups):
        for copy in text_copies[g]:
            copy.wait()
        for i in range(per):
            h = g * per + i
            cols = slice(i * size, (i + 1) * size)
            key = tk_buf[g, :, cols].astype(jnp.float32)
            key = (key * rsqrt_mean(key) * tkg_ref[...]).astype(jnp.bfloat16)
            scores = jnp.where(valid, scores_of(qs[h], key), LOW)
            top = jnp.max(scores, axis=-1, keepdims=True)
            expo = jnp.where(valid, jnp.exp2(scores - top), 0.0)
            m_buf[h] = jnp.broadcast_to(top, (rows, size))
            l_buf[h] = jnp.broadcast_to(jnp.sum(expo, axis=-1, keepdims=True), (rows, size))
            o_buf[h] = jnp.dot(
                expo.astype(jnp.bfloat16),
                tv_buf[g, :, cols],
                preferred_element_type=jnp.float32,
            )
        for task in stages[g]:
            task()

    for z in [z_me] + z_others:
        for y in [y_me] + y_others:
            for x in x_others:
                arrive(0, block(z, y, x))
        for x in [x_me] + x_others:
            for y in y_others:
                arrive(1, block(z, y, x))

    def lanes(h):
        return slice(h * size, (h + 1) * size)

    def gathered(buf, h):
        whole = buf[:, :, lanes(h)].astype(jnp.float32)
        return whole.reshape(devices * own_rows, size).astype(jnp.bfloat16)

    every = range(heads)
    scores = [scores_of(qs[h], gathered(kbuf, h)) for h in every]
    olds = [m_buf[h] for h in every]
    tops = [
        jnp.maximum(olds[h][:, :1], jnp.max(scores[h], axis=-1, keepdims=True))
        for h in every
    ]
    expos = [jnp.exp2(scores[h] - tops[h]) for h in every]
    added = [
        jnp.dot(
            expos[h].astype(jnp.bfloat16),
            gathered(vbuf, h),
            preferred_element_type=jnp.float32,
        )
        for h in every
    ]
    sums = [jnp.sum(expos[h], axis=-1, keepdims=True) for h in every]
    for h in every:
        back = jnp.exp2(olds[h] - tops[h])
        out = (o_buf[h] * back + added[h]) / (l_buf[h] * back + sums[h])
        to_ref[:, lanes(h)] = out[:share].astype(jnp.bfloat16)
        io_ref[:, lanes(h)] = out[share:].astype(jnp.bfloat16)

    for copy in sends:
        copy.wait_send()


def send_count(devices):
    zs, ys, xs = line_sizes(devices)
    keys = (zs - 1) + zs * (ys - 1) + zs * ys * (xs - 1)
    values = (zs - 1) + zs * (xs - 1) + zs * xs * (ys - 1)
    return keys + values


def local(iq, ik, iv, tq, tk, tv, iqg, ikg, tqg, tkg, order, length):
    devices = lax.axis_size("seq")
    own_rows, width = iq.shape
    size = iqg.shape[0]
    heads = width // size
    text_rows = tq.shape[0]
    share = text_rows // devices
    rows = share + own_rows
    groups = heads // 2 if heads % 2 == 0 else heads
    span = width // groups
    vmem = pl.BlockSpec(memory_space=pltpu.VMEM)
    smem = pl.BlockSpec(memory_space=pltpu.SMEM)
    hbm = pl.BlockSpec(memory_space=pl.ANY)
    gains = [g.reshape(1, size) for g in (iqg, ikg, tqg, tkg)]
    return pl.pallas_call(
        functools.partial(kernel, devices),
        out_shape=(
            jax.ShapeDtypeStruct((own_rows, width), jnp.bfloat16),
            jax.ShapeDtypeStruct((share, width), jnp.bfloat16),
        ),
        in_specs=[vmem] * 3 + [hbm] * 3 + [vmem] * 4 + [smem] * 2,
        out_specs=(vmem, vmem),
        scratch_shapes=[
            pltpu.VMEM((devices, own_rows, width), jnp.bfloat16),
            pltpu.VMEM((devices, own_rows, width), jnp.bfloat16),
            pltpu.VMEM((share, width), jnp.bfloat16),
            pltpu.VMEM((groups, text_rows, span), jnp.bfloat16),
            pltpu.VMEM((groups, text_rows, span), jnp.bfloat16),
            pltpu.VMEM((heads, rows, size), jnp.bfloat16),
            pltpu.VMEM((heads, rows, size), jnp.float32),
            pltpu.VMEM((heads, rows, size), jnp.float32),
            pltpu.VMEM((heads, rows, size), jnp.float32),
            pltpu.SemaphoreType.DMA((2, devices)),
            pltpu.SemaphoreType.DMA((send_count(devices),)),
            pltpu.SemaphoreType.DMA((2 * groups + 1,)),
        ],
        compiler_params=pltpu.CompilerParams(
            collective_id=0, has_side_effects=True, vmem_limit_bytes=62 * 1024 * 1024
        ),
    )(iq, ik, iv, tq, tk, tv, *gains, order, length)


def solution(mesh):
    rows = P(("req", "seq"), None)
    text = P("req", None)
    return jax.shard_map(
        local,
        mesh=mesh,
        in_specs=(rows, rows, rows, text, text, text)
        + (P(), P(), P(), P(), P(("req", "seq")), P("req")),
        out_specs=(rows, rows),
        check_vma=False,
    )
```
